32 devices in a mesh: src: 8 (over z, x), dst: 4 (over y, core).
Axes of the slice: x: 2, y: 2, z: 4, core: 2. Of those that a mesh axis runs over, the one named last changes fastest.
Arguments:
- counts: int32 [8, 2048, 4096], P(None, 'src', 'dst'), may hold values from 0 to 63
- src_factor: float32 [2048, 128], P('src'), may hold values from 0.25 to 32
- dst_factor: float32 [4096, 128], P('dst'), may hold values from 0.25 to 32
- hour_factor: float32 [8, 32], replicated, may hold values from 0.25 to 4
- core: float32 [32, 128, 128], replicated, may hold values from 1e-06 to 1e-05
Outputs:
- grad_src: float32 [2048, 128], P('src')
- grad_dst: float32 [4096, 128], P('dst')
- grad_hour: float32 [8, 32], replicated
- grad_core: float32 [32, 128, 128], P(None, 'src')
The draws below stay inside these ranges and needn't reach their ends.
All inputs are finite; a program needn't handle non-finite values.
Results may differ from the reference program's by a relative error of at most 0.0003.
Values sent between devices are 32-bit elements; how exact they have to be, the bound alone decides.
A program may use at most 64 MiB of HBM per device.

```python
import math
import jax
import jax.numpy as jnp
from jax import lax

HOURS = 8
R1 = 128
R2 = 128
R3 = 32
I = 2048
J = 4096
N_SRC = 8


def row_groups(key, salt, number):
    return jax.random.randint(jax.random.fold_in(key, salt), (number,), 0, 8).astype(jnp.int32)


def boosted(base, groups, width):
    columns = jnp.arange(width, dtype=jnp.int32) % 8
    boost = jnp.where(columns[None, :] == groups[:, None], 8.0, 1.0).astype(jnp.float32)
    return (base * boost).astype(jnp.float32)


def draw_counts(key, part):
    src_groups = row_groups(key, 11, I)
    dst_groups = row_groups(key, 12, J)
    levels = jax.random.randint(jax.random.fold_in(key, 13), (8, 8), 12, 65).astype(jnp.int32)
    src_levels = jnp.take(levels, src_groups, axis=0)
    pair_level = jnp.take(src_levels, dst_groups, axis=1)
    raw_counts = jax.random.randint(jax.random.fold_in(key, 14), (HOURS, I, J), 0, 64).astype(jnp.int32)
    return jnp.minimum(raw_counts * pair_level[None, :, :] // 48, 63).astype(jnp.int32)


def draw_src_factor(key, part):
    groups = row_groups(key, 11, I)
    sub_key = jax.random.fold_in(key, 21)
    base = jnp.exp(jax.random.uniform(sub_key, (I, R1), jnp.float32, jnp.log(0.25), jnp.log(4.0)))
    return boosted(base, groups, R1)


def draw_dst_factor(key, part):
    groups = row_groups(key, 12, J)
    sub_key = jax.random.fold_in(key, 22)
    base = jnp.exp(jax.random.uniform(sub_key, (J, R2), jnp.float32, jnp.log(0.25), jnp.log(4.0)))
    return boosted(base, groups, R2)


def setup_inputs(seed: int = 0) -> dict:
    keys = jax.random.split(jax.random.key(seed), 6)
    return {
        "counts": draw_counts(jax.random.fold_in(keys[5], 71), 0),
        "src_factor": draw_src_factor(jax.random.fold_in(keys[5], 71), 0),
        "dst_factor": draw_dst_factor(jax.random.fold_in(keys[5], 71), 0),
        "hour_factor": jnp.clip(jnp.exp(jax.random.uniform(keys[3], (HOURS, R3), jnp.float32, math.log(0.25), math.log(4.0))), 0.25, 4.0),
        "core": jnp.clip(jnp.exp(jax.random.uniform(keys[4], (R3, R1, R2), jnp.float32, math.log(9.999999974752427e-07), math.log(9.999999747378752e-06))), 9.999999974752427e-07, 9.999999747378752e-06),
    }


def reference(counts, src_factor, dst_factor, hour_factor, core):
    highest = lax.Precision.HIGHEST
    core_hours = jnp.einsum('kr,rpq->kpq', hour_factor, core, precision=highest)
    row_count = I // N_SRC

    def block_step(totals, block_index):
        offset = (block_index * row_count).astype(jnp.int32)
        block_counts = lax.dynamic_slice_in_dim(counts, offset, row_count, 1).astype(jnp.float32)
        block_src = lax.dynamic_slice_in_dim(src_factor, offset, row_count, 0)
        partial_fit = jnp.einsum('ip,kpq->kiq', block_src, core_hours, precision=highest)
        fitted = jnp.einsum('kiq,jq->kij', partial_fit, dst_factor, precision=highest)
        misfit = 1.0 - block_counts / fitted
        dst_sum = totals[0] + jnp.einsum('kij,kiq->jq', misfit, partial_fit, precision=highest)
        through = jnp.einsum('kij,jq->kiq', misfit, dst_factor, precision=highest)
        src_block = jnp.einsum('kiq,kpq->ip', through, core_hours, precision=highest)
        projected = totals[1] + jnp.einsum('ip,kiq->kpq', block_src, through, precision=highest)
        return ((dst_sum, projected), src_block)
    start_totals = (jnp.zeros((J, R2), jnp.float32), jnp.zeros((HOURS, R1, R2), jnp.float32))
    (dst_sum, projected), src_blocks = lax.scan(block_step, start_totals, jnp.arange(N_SRC, dtype=jnp.int32))
    grad_src = src_blocks.reshape(I, R1) / math.sqrt(J * HOURS)
    grad_dst = dst_sum / math.sqrt(I * HOURS)
    grad_hour = jnp.einsum('kpq,rpq->kr', projected, core, precision=highest) / math.sqrt(I * J)
    grad_core = jnp.einsum('kr,kpq->rpq', hour_factor, projected, precision=highest) / math.sqrt(I * J * HOURS)
    return (grad_src, grad_dst, grad_hour, grad_core)
```

```python
import functools
import math

import jax
import jax.numpy as jnp
from jax import lax
from jax.experimental import pallas as pl
from jax.experimental.pallas import tpu as pltpu
from jax.sharding import PartitionSpec as P

F32 = jnp.float32
BF16 = jnp.bfloat16
MESH = pl.DeviceIdType.MESH


def split(x):
    hi = x.astype(BF16)
    lo = (x - hi.astype(F32)).astype(BF16)
    return hi, lo


def dg(a, b, ca, cb):
    return lax.dot_general(a, b, (((ca,), (cb,)), ((), ())), preferred_element_type=F32)


def dot3(a, b, ca, cb):
    ah, al = a
    bh, bl = b
    return dg(ah, bh, ca, cb) + dg(ah, bl, ca, cb) + dg(al, bh, ca, cb)


def kernel(
    n, nz, nx, nd, nh, tj,
    counts, src_in, dst_in, hour, core_in,
    g_src, g_dst, g_hour, g_core,
    src, dst, core, cnt, ch, pf_ks, pf_t, d_k, d_n, thr, dacc, r1, r2,
    chs, gterm, r3, proj, q1, q2, pq, q3, pk, hacc, hd, hs, msc, accr,
    i_sem, c_sem, s1s, s1r, s2s, s2r, zs, zr, xs, xr,
    gs1s, gs1r, gs2s, gs2r, q1s, q1r, q2s, q2r, q3s, q3r, pks, pkr, hds, hdr, hss, hsr,
):
    s = lax.axis_index("src")
    d = lax.axis_index("dst")
    a = s // nx
    b = lax.rem(s, nx)
    yy = d // 2
    cc = lax.rem(d, 2)
    ny = nd // 2
    kk, ni, _ = counts.shape
    nj = dst.shape[0]
    r3n = core.shape[0]
    r1n = core.shape[1]
    r2n = dst.shape[1]
    half = nj // nx
    zrows = tj // nz
    kd = kk // nd
    share = r1n // n
    irows = ni // nd
    nt = nh * nx
    scale_src = 1.0 / math.sqrt(nj * nd * kk)
    scale_dst = 1.0 / math.sqrt(ni * n * kk)
    scale_hour = 1.0 / math.sqrt(ni * n * nj * nd)
    scale_core = 1.0 / math.sqrt(ni * n * nj * nd * kk)

    dst_copy = pltpu.make_async_copy(dst_in, dst, i_sem.at[0])
    core_copy = pltpu.make_async_copy(core_in, core, i_sem.at[1])
    src_copy = pltpu.make_async_copy(src_in, src, i_sem.at[2])
    for c in (dst_copy, core_copy, src_copy):
        c.start()

    def block_start(t):
        return lax.rem(b + 1 + t % nx, nx) * half + (t // nx) * tj

    def count_copy(t):
        start = pl.multiple_of(block_start(t), tj)
        return pltpu.make_async_copy(counts.at[:, :, pl.ds(start, tj)], cnt.at[t], c_sem.at[t])

    for t in range(nt):
        count_copy(t).start()

    barrier = pltpu.get_barrier_semaphore()
    for o in range(1, n):
        pl.semaphore_signal(barrier, inc=1, device_id={"src": lax.rem(s + o, n)}, device_id_type=MESH)
    for o in range(1, nd):
        pl.semaphore_signal(barrier, inc=1, device_id={"dst": lax.rem(d + o, nd)}, device_id_type=MESH)

    def rc(src_ref, dst_ref, send, recv, **where):
        return pltpu.make_async_remote_copy(
            src_ref=src_ref, dst_ref=dst_ref, send_sem=send, recv_sem=recv,
            device_id=where, device_id_type=MESH,
        )

    dst_copy.wait()
    dh, dl = split(dst[...])
    d_n[...] = jnp.concatenate([dh, dl], axis=1)
    dth, dtl = split(dst[...].T)
    d_k[...] = jnp.concatenate([dth, dth, dtl], axis=0)
    thr[...] = jnp.zeros_like(thr)
    accr[...] = jnp.zeros_like(accr)

    core_copy.wait()
    pt = 32

    def core_tile(i, carry):
        at = pl.ds(pl.multiple_of(i * pt, pt), pt)
        accs = [None] * kk
        for r in range(r3n):
            tile = core[r, at, :]
            for k in range(kk):
                term = tile * hour[k, r]
                accs[k] = term if r == 0 else accs[k] + term
        for k in range(kk):
            ch[k, at, :] = accs[k]
        return carry

    lax.fori_loop(0, r1n // pt, core_tile, 0)

    src_copy.wait()
    src_parts = split(src[...])

    def fit_one(k, carry):
        chh, chl = split(ch[k])
        chs[k] = jnp.concatenate([chh, chh, chl], axis=1)
        pf = dot3(src_parts, (chh, chl), 1, 0)
        ph, plo = split(pf)
        pf_ks[k] = jnp.concatenate([ph, plo, ph], axis=1)
        th, tl = split(pf.T)
        pf_t[k] = jnp.concatenate([th, tl], axis=0)
        return carry

    lax.fori_loop(0, kk, fit_one, 0)
    sth, stl = split(src[...].T)

    def misfit(t, start, k, slot):
        at = pl.ds(pl.multiple_of(start, tj), tj)
        fitted = dg(pf_ks[pl.ds(k, kd)].reshape(kd * ni, 3 * r2n), d_k[:, at], 1, 0)
        m = 1.0 - cnt[t, pl.ds(k, kd)].reshape(kd * ni, tj).astype(F32) / fitted
        mh, ml = split(m)
        msc[slot, 0] = mh
        msc[slot, 1] = ml

    def gather_terms(start, k, slot):
        dn = d_n[pl.ds(pl.multiple_of(start, tj), tj), :]
        mh = msc[slot, 0]
        ml = msc[slot, 1]
        wide = dg(mh, dn, 1, 0)
        new = thr[pl.ds(k, kd)].reshape(kd * ni, r2n) + (wide[:, :r2n] + wide[:, r2n:] + dg(ml, dn[:, :r2n], 1, 0))
        thr[pl.ds(k, kd)] = new.reshape(kd, ni, r2n)
        acc = accr[...]
        for e in range(kd):
            pt_ = pf_t[k + e]
            rows = slice(e * ni, (e + 1) * ni)
            tall = dg(pt_, mh[rows], 1, 0)
            acc = acc + (tall[:r2n] + tall[r2n:] + dg(pt_[:r2n], ml[rows], 1, 0))
        accr[...] = acc
        return new

    groups = [(side, oy) for side in (1, 0) for oy in list(range(1, ny)) + [0]]

    def group_first(g):
        side, oy = groups[g]
        return (2 * lax.rem(yy + oy, ny) + lax.rem(cc + side, 2)) * kd

    first_hour = group_first(0)
    pairs = kk // (2 * kd)

    def compute_block(t):
        count_copy(t + 1).wait()
        start = block_start(t)
        after = block_start(t + 1)
        after_k = first_hour if t + 1 == nt - 1 else 0

        def two(i, carry):
            k = 2 * kd * i
            misfit(t, start, k + kd, 1)
            gather_terms(start, k, 0)
            end = (i + 1) // pairs
            misfit(t + end, start + end * (after - start), (1 - end) * (k + 2 * kd) + end * after_k, 0)
            gather_terms(start, k + kd, 1)
            return carry

        lax.fori_loop(0, pairs, two, 0)
        dacc[pl.ds(pl.multiple_of(start, tj), tj), :] = accr[...].T
        accr[...] = jnp.zeros_like(accr)

    s1, s2, zc, xc = [], [], {}, []

    def x_send(t):
        h, step = t // nx, t % nx
        at = pl.ds(pl.multiple_of(block_start(t), tj), tj)
        slot = h * (nx - 1) + step
        c = rc(dacc.at[at, :], r1.at[slot], s1s.at[slot], s1r.at[slot], src=a * nx + lax.rem(b + 1 + step, nx))
        c.start()
        s1.append(c)

    def z_piece(h, owner):
        return pl.ds(pl.multiple_of(b * half + h * tj + owner * zrows, zrows), zrows)

    def z_send(h):
        own = pl.ds(pl.multiple_of(b * half + h * tj, tj), tj)
        value = dacc[own, :]
        for step in range(nx - 1):
            s1[h * (nx - 1) + step].wait_recv()
            value = value + r1[h * (nx - 1) + step]
        dacc[own, :] = value
        for o in range(1, nz):
            owner = lax.rem(a + o, nz)
            slot = h * (nz - 1) + o - 1
            c = rc(dacc.at[z_piece(h, owner), :], r2.at[slot], s2s.at[slot], s2r.at[slot], src=owner * nx + b)
            c.start()
            s2.append(c)

    def x_copy(h, step, o):
        at = z_piece(h, lax.rem(a - o + nz, nz))
        slot = (h * (nx - 1) + step) * nz + o
        return rc(g_dst.at[at, :], g_dst.at[at, :], xs.at[slot], xr.at[slot],
                  src=a * nx + lax.rem(b + 1 + step, nx))

    def x_forward(h, o):
        for step in range(nx - 1):
            c = x_copy(h, step, o)
            c.start()
            xc.append(c)

    def finish(h):
        mine = z_piece(h, a)
        total = dacc[mine, :]
        for o in range(1, nz):
            s2[h * (nz - 1) + o - 1].wait_recv()
            total = total + r2[h * (nz - 1) + o - 1]
        g_dst[mine, :] = total * scale_dst
        x_forward(h, 0)
        for o in range(1, nz):
            slot = h * (nz - 1) + o - 1
            c = rc(g_dst.at[mine, :], g_dst.at[mine, :], zs.at[slot], zr.at[slot], src=lax.rem(a + o, nz) * nx + b)
            c.start()
            zc[h, o] = c

    def forward(h):
        for o in range(1, nz):
            zc[h, o].wait_recv()
            x_forward(h, o)

    q1c, q2c = [], []

    def last_block(t):
        start = block_start(t)
        gacc = None
        for g, (side, oy) in enumerate(groups):
            slot = g % 2
            first = group_first(g)
            if g + 1 < nd:
                misfit(t, start, group_first(g + 1), 1 - slot)
            new = gather_terms(start, first, slot)
            th, tl = split(new)
            for e in range(kd):
                rows = slice(e * ni, (e + 1) * ni)
                wide = dg(sth, jnp.concatenate([th[rows], tl[rows]], axis=1), 1, 0)
                proj[first + e] = wide[:, :r2n] + wide[:, r2n:] + dg(stl, th[rows], 1, 0)
                term = dg(jnp.concatenate([th[rows], tl[rows], th[rows]], axis=1), chs[first + e], 1, 1)
                gacc = term if gacc is None else gacc + term
            core_of = lax.rem(cc + side, 2)
            peer = lax.rem(yy + oy, ny)
            if side:
                c = rc(proj.at[pl.ds(first, kd)], q1.at[peer], q1s.at[oy], q1r.at[oy], dst=2 * yy + core_of)
                c.start()
                q1c.append(c)
            else:
                q1c[oy - 1 if oy else ny - 1].wait_recv()
                q1[peer] = q1[peer] + proj[pl.ds(first, kd)]
                if oy:
                    c = rc(q1.at[peer], q2.at[oy - 1], q2s.at[oy - 1], q2r.at[oy - 1], dst=2 * peer + cc)
                    c.start()
                    q2c.append(c)
            if g == nd // 2 - 1:
                for h in range(nh - 1):
                    z_send(h)
        gterm[...] = gacc
        dacc[pl.ds(pl.multiple_of(start, tj), tj), :] = accr[...].T

    count_copy(0).wait()
    misfit(0, block_start(0), 0 if nt > 1 else first_hour, 0)
    for t in range(nt - 1):
        compute_block(t)
        if t == 0:
            pl.semaphore_wait(barrier, n - 1 + nd - 1)
        if t % nx < nx - 1:
            x_send(t)
    last_block(nt - 1)

    g1 = []
    for o in range(1, nd):
        peer = lax.rem(d + o, nd)
        c = rc(gterm.at[pl.ds(pl.multiple_of(peer * irows, irows), irows), :], r3.at[o - 1], gs1s.at[o - 1], gs1r.at[o - 1],
               dst=peer)
        c.start()
        g1.append(c)

    z_send(nh - 1)

    ysum = q1[yy]
    for o in range(1, ny):
        q2c[o - 1].wait_recv()
        ysum = ysum + q2[o - 1]
    for i in range(n):
        pq[i] = ysum[:, i * share:(i + 1) * share, :]
    q3c = []
    for o in range(1, n):
        peer = lax.rem(s + o, n)
        c = rc(pq.at[peer], q3.at[o - 1], q3s.at[o - 1], q3r.at[o - 1], src=peer)
        c.start()
        q3c.append(c)

    for h in range(nh - 1):
        finish(h)

    def hour_row(r, carry):
        for k in range(kk):
            acc = core[r, 0:8, :] * proj[k, 0:8, :]
            for i in range(1, r1n // 8):
                acc = acc + core[r, 8 * i:8 * i + 8, :] * proj[k, 8 * i:8 * i + 8, :]
            hacc[k, r] = acc
        return carry

    lax.fori_loop(0, r3n, hour_row, 0)
    hl = jnp.sum(jnp.sum(hacc[...], axis=2), axis=2)
    hl = jnp.concatenate([hl, jnp.zeros((kk, hd.shape[2] - r3n), F32)], axis=1)
    hd[d] = hl
    h1 = []
    for o in range(1, nd):
        c = rc(hd.at[d], hd.at[d], hds.at[o - 1], hdr.at[o - 1], dst=lax.rem(d + o, nd))
        c.start()
        h1.append(c)

    own_rows = pl.ds(pl.multiple_of(d * irows, irows), irows)
    gsum = gterm[own_rows, :]
    for o in range(1, nd):
        g1[o - 1].wait_recv()
        gsum = gsum + r3[o - 1]
    g_src[own_rows, :] = gsum * scale_src
    g2 = []
    for o in range(1, nd):
        c = rc(g_src.at[own_rows, :], g_src.at[own_rows, :], gs2s.at[o - 1], gs2r.at[o - 1], dst=lax.rem(d + o, nd))
        c.start()
        g2.append(c)

    finish(nh - 1)

    for o in range(1, nd):
        h1[o - 1].wait_recv()
    hsum = hd[0]
    for i in range(1, nd):
        hsum = hsum + hd[i]
    hs[s] = hsum
    h2 = []
    for o in range(1, n):
        c = rc(hs.at[s], hs.at[s], hss.at[o - 1], hsr.at[o - 1], src=lax.rem(s + o, n))
        c.start()
        h2.append(c)

    psum = pq[s]
    for o in range(1, n):
        q3c[o - 1].wait_recv()
        psum = psum + q3[o - 1]
    pk[d] = psum
    pkc = []
    for o in range(1, nd):
        c = rc(pk.at[d], pk.at[d], pks.at[o - 1], pkr.at[o - 1], dst=lax.rem(d + o, nd))
        c.start()
        pkc.append(c)

    for h in range(nh):
        forward(h)

    for o in range(1, n):
        h2[o - 1].wait_recv()
    htot = hs[0]
    for i in range(1, n):
        htot = htot + hs[i]
    g_hour[...] = htot[:, :r3n] * scale_hour

    for o in range(1, nd):
        pkc[o - 1].wait_recv()
    tiles = [pk[k // kd, k % kd] * scale_core for k in range(kk)]
    for r in range(r3n):
        acc = tiles[0] * hour[0, r]
        for k in range(1, kk):
            acc = acc + tiles[k] * hour[k, r]
        g_core[r] = acc

    for c in g2:
        c.wait_recv()
    for c in xc:
        c.wait_recv()
    for c in s1 + s2 + list(zc.values()) + xc + g1 + g2 + q1c + q2c + q3c + pkc + h1 + h2:
        c.wait_send()


def write_out(*refs):
    half = len(refs) // 3
    ins, outs, sems = refs[:half], refs[half:2 * half], refs[2 * half:]
    copies = [pltpu.make_async_copy(i, o, m) for i, o, m in zip(ins, outs, sems)]
    for c in copies:
        c.start()
    for c in copies:
        c.wait()


def solution(mesh):
    n = mesh.shape["src"]
    nd = mesh.shape["dst"]
    nx = 2 ** (int(math.log2(n)) // 2)
    nz = n // nx
    ny = nd // 2

    def shards(counts, src, dst, hour, core):
        kk, ni, nj = counts.shape
        r3n, r1n, r2n = core.shape
        tj = min(256, nj // nx)
        nh = nj // (nx * tj)
        kd = kk // nd
        share = r1n // n
        irows = ni // nd
        vm = pl.BlockSpec(memory_space=pltpu.VMEM)
        hbm = pl.BlockSpec(memory_space=pl.ANY)
        dma = lambda *shape: pltpu.SemaphoreType.DMA(shape)
        f = lambda *shape: pltpu.VMEM(shape, F32)
        h = lambda *shape: pltpu.VMEM(shape, BF16)
        pair = lambda m: [dma(m), dma(m)]
        scratch = [
            f(ni, r1n), f(nj, r2n), f(r3n, r1n, r2n), pltpu.VMEM((nh * nx, kk, ni, tj), jnp.int32),
            f(kk, r1n, r2n), h(kk, ni, 3 * r2n), h(kk, 2 * r2n, ni), h(3 * r2n, nj), h(nj, 2 * r2n),
            f(kk, ni, r2n), f(nj, r2n), f(nh * (nx - 1), tj, r2n), f(nh * (nz - 1), tj // nz, r2n),
            h(kk, r1n, 3 * r2n), f(ni, r1n), f(nd - 1, irows, r1n), f(kk, r1n, r2n), f(ny, kd, r1n, r2n), f(ny - 1, kd, r1n, r2n),
            f(n, kd, share, r2n), f(n - 1, kd, share, r2n), f(nd, kd, share, r2n), f(kk, r3n, 8, r2n),
            f(nd, kk, 128), f(n, kk, 128), h(2, 2, kd * ni, tj), f(r2n, tj),
            dma(3), dma(nh * nx),
        ]
        for m in (nh * (nx - 1), nh * (nz - 1), nh * (nz - 1), nh * (nx - 1) * nz, nd - 1, nd - 1, ny, ny - 1, n - 1, nd - 1, nd - 1, n - 1):
            scratch += pair(m)
        shapes = ((ni, r1n), (nj, r2n), (kk, r3n), (r3n, share, r2n))
        results = pl.pallas_call(
            functools.partial(kernel, n, nz, nx, nd, nh, tj),
            out_shape=tuple(pltpu.VMEM(x, F32) for x in shapes),
            in_specs=[hbm, hbm, hbm, pl.BlockSpec(memory_space=pltpu.SMEM), hbm],
            out_specs=(vm, vm, vm, vm),
            scratch_shapes=scratch,
            compiler_params=pltpu.CompilerParams(
                collective_id=0, has_side_effects=True, vmem_limit_bytes=60 * 1024 * 1024
            ),
        )(counts, src, dst, hour, core)
        return pl.pallas_call(
            write_out,
            out_shape=tuple(jax.ShapeDtypeStruct(x, F32) for x in shapes),
            in_specs=[vm] * 4,
            out_specs=(pl.BlockSpec(memory_space=pl.ANY),) * 4,
            scratch_shapes=[pltpu.SemaphoreType.DMA] * 4,
        )(*(pltpu.with_memory_space_constraint(x, pltpu.VMEM) for x in results))

    in_specs = (P(None, "src", "dst"), P("src", None), P("dst", None), P(), P())
    out_specs = (P("src", None), P("dst", None), P(), P(None, "src", None))
    return jax.shard_map(shards, mesh=mesh, in_specs=in_specs, out_specs=out_specs, check_vma=False)
```

```python
import functools
import math

import jax
import jax.numpy as jnp
from jax import lax
from jax.experimental import pallas as pl
from jax.experimental.pallas import tpu as pltpu
from jax.sharding import PartitionSpec as P

F32 = jnp.float32
BF16 = jnp.bfloat16
MESH = pl.DeviceIdType.MESH


def split(x):
    hi = x.astype(BF16)
    lo = (x - hi.astype(F32)).astype(BF16)
    return hi, lo


def dg(a, b, ca, cb):
    return lax.dot_general(a, b, (((ca,), (cb,)), ((), ())), preferred_element_type=F32)


def dot3(a, b, ca, cb):
    ah, al = a
    bh, bl = b
    return dg(ah, bh, ca, cb) + dg(ah, bl, ca, cb) + dg(al, bh, ca, cb)


def kernel(
    n, nz, nx, nd, nh, tj,
    counts, src_in, dst_in, hour, core_in,
    g_src, g_dst, g_hour, g_core,
    src, dst, core, cnt, ch, pf_ks, pf_t, d_k, d_n, thr, dacc, r1, r2,
    chs, gterm, r3, proj, q1, q2, pq, q3, pk, hacc, hd, hs, msc,
    i_sem, c_sem, s1s, s1r, s2s, s2r, zs, zr, xs, xr,
    gs1s, gs1r, gs2s, gs2r, q1s, q1r, q2s, q2r, q3s, q3r, pks, pkr, hds, hdr, hss, hsr,
):
    s = lax.axis_index("src")
    d = lax.axis_index("dst")
    a = s // nx
    b = lax.rem(s, nx)
    yy = d // 2
    cc = lax.rem(d, 2)
    ny = nd // 2
    kk, ni, _ = counts.shape
    nj = dst.shape[0]
    r3n = core.shape[0]
    r1n = core.shape[1]
    r2n = dst.shape[1]
    half = nj // nx
    zrows = tj // nz
    kd = kk // nd
    share = r1n // n
    irows = ni // nd
    nt = nh * nx
    scale_src = 1.0 / math.sqrt(nj * nd * kk)
    scale_dst = 1.0 / math.sqrt(ni * n * kk)
    scale_hour = 1.0 / math.sqrt(ni * n * nj * nd)
    scale_core = 1.0 / math.sqrt(ni * n * nj * nd * kk)

    dst_copy = pltpu.make_async_copy(dst_in, dst, i_sem.at[0])
    core_copy = pltpu.make_async_copy(core_in, core, i_sem.at[1])
    src_copy = pltpu.make_async_copy(src_in, src, i_sem.at[2])
    for c in (dst_copy, core_copy, src_copy):
        c.start()

    def block_start(t):
        return lax.rem(b + 1 + t // nh, nx) * half + (t % nh) * tj

    def flip(e):
        out = a
        for bit in range(e.bit_length()):
            if (e >> bit) % 2:
                out = out + (1 << bit) * (1 - 2 * lax.rem(a // (1 << bit), 2))
        return out

    far_first = list(range(nz - 1, 0, -1))

    def count_copy(t):
        start = pl.multiple_of(block_start(t), tj)
        return pltpu.make_async_copy(counts.at[:, :, pl.ds(start, tj)], cnt.at[t], c_sem.at[t])

    for t in range(nt):
        count_copy(t).start()

    barrier = pltpu.get_barrier_semaphore()
    for o in range(1, n):
        pl.semaphore_signal(barrier, inc=1, device_id={"src": lax.rem(s + o, n)}, device_id_type=MESH)
    for o in range(1, nd):
        pl.semaphore_signal(barrier, inc=1, device_id={"dst": lax.rem(d + o, nd)}, device_id_type=MESH)

    def rc(src_ref, dst_ref, send, recv, **where):
        return pltpu.make_async_remote_copy(
            src_ref=src_ref, dst_ref=dst_ref, send_sem=send, recv_sem=recv,
            device_id=where, device_id_type=MESH,
        )

    dst_copy.wait()
    dh, dl = split(dst[...])
    d_n[...] = jnp.concatenate([dh, dl], axis=1)
    dth, dtl = split(dst[...].T)
    d_k[...] = jnp.concatenate([dth, dth, dtl], axis=0)

    core_copy.wait()
    pt = 32

    def core_tile(i, carry):
        at = pl.ds(pl.multiple_of(i * pt, pt), pt)
        accs = [None] * kk
        for r in range(r3n):
            tile = core[r, at, :]
            for k in range(kk):
                term = tile * hour[k, r]
                accs[k] = term if r == 0 else accs[k] + term
        for k in range(kk):
            ch[k, at, :] = accs[k]
        return carry

    lax.fori_loop(0, r1n // pt, core_tile, 0)

    src_copy.wait()
    src_parts = split(src[...])

    def fit_one(k, carry):
        chh, chl = split(ch[k])
        chs[k] = jnp.concatenate([chh, chh, chl], axis=1)
        pf = dot3(src_parts, (chh, chl), 1, 0)
        ph, plo = split(pf)
        pf_ks[k] = jnp.concatenate([ph, plo, ph], axis=1)
        th, tl = split(pf.T)
        pf_t[k] = jnp.concatenate([th, tl], axis=0)
        return carry

    lax.fori_loop(0, kk, fit_one, 0)
    sth, stl = split(src[...].T)

    def misfit(t, g):
        at = pl.ds(pl.multiple_of(block_start(t), tj), tj)
        hours = slice(g * kd, (g + 1) * kd)
        fitted = dg(pf_ks[hours].reshape(kd * ni, 3 * r2n), d_k[:, at], 1, 0)
        m = 1.0 - cnt[t, hours].reshape(kd * ni, tj).astype(F32) / fitted
        mh, ml = split(m)
        msc[t, g, 0] = mh
        msc[t, g, 1] = ml

    def add_tall(t, g, acc):
        for e in range(kd):
            pt_ = pf_t[g * kd + e]
            rows = slice(e * ni, (e + 1) * ni)
            tall = dg(pt_, msc[t, g, 0, rows], 1, 0)
            new = tall[:r2n] + tall[r2n:] + dg(pt_[:r2n], msc[t, g, 1, rows], 1, 0)
            acc = new if acc is None else acc + new
        return acc

    def through(gi):
        out = None
        for t in range(nt):
            dn = d_n[pl.ds(pl.multiple_of(block_start(t), tj), tj), :]
            wide = dg(msc[t, gi, 0], dn, 1, 0)
            new = wide[:, :r2n] + wide[:, r2n:] + dg(msc[t, gi, 1], dn[:, :r2n], 1, 0)
            out = new if out is None else out + new
        return out

    groups = [(side, oy) for side in (1, 0) for oy in list(range(1, ny)) + [0]]

    def group_of(g):
        side, oy = groups[g]
        return 2 * lax.rem(yy + oy, ny) + lax.rem(cc + side, 2)

    def compute_block(t):
        if t + 1 < nt:
            count_copy(t + 1).wait()
        acc = None
        for g in range(nd):
            if g + 1 < nd:
                misfit(t, g + 1)
            elif t + 1 < nt:
                misfit(t + 1, 0)
            acc = add_tall(t, g, acc)
        dacc[pl.ds(pl.multiple_of(block_start(t), tj), tj), :] = acc.T

    s1, s2, zc, xc = {}, {}, {}, []

    def x_send(h, step):
        start = block_start(step * nh + h)
        slot = h * (nx - 1) + step
        for e in far_first + [0]:
            at = flip(e) * zrows
            c = rc(dacc.at[pl.ds(pl.multiple_of(start + at, zrows), zrows), :],
                   r1.at[slot, pl.ds(pl.multiple_of(at, zrows), zrows), :],
                   s1s.at[slot * nz + e], s1r.at[slot * nz + e], src=a * nx + lax.rem(b + 1 + step, nx))
            c.start()
            s1[slot, e] = c

    def z_piece(h, owner):
        return pl.ds(pl.multiple_of(b * half + h * tj + owner * zrows, zrows), zrows)

    def z_send(h, e):
        owner = flip(e)
        at = z_piece(h, owner)
        value = dacc[at, :]
        for step in range(nx - 1):
            s1[h * (nx - 1) + step, e].wait_recv()
            value = value + r1[h * (nx - 1) + step, pl.ds(pl.multiple_of(owner * zrows, zrows), zrows), :]
        dacc[at, :] = value
        if e:
            slot = h * (nz - 1) + e - 1
            c = rc(dacc.at[at, :], r2.at[slot], s2s.at[slot], s2r.at[slot], src=owner * nx + b)
            c.start()
            s2[h, e] = c

    def x_copy(h, step, o):
        at = z_piece(h, flip(o))
        slot = (h * (nx - 1) + step) * nz + o
        return rc(g_dst.at[at, :], g_dst.at[at, :], xs.at[slot], xr.at[slot],
                  src=a * nx + lax.rem(b + 1 + step, nx))

    def x_forward(h, o):
        for step in range(nx - 1):
            c = x_copy(h, step, o)
            c.start()
            xc.append(c)

    def finish(h):
        mine = z_piece(h, a)
        total = dacc[mine, :]
        for e in far_first:
            s2[h, e].wait_recv()
            total = total + r2[h * (nz - 1) + e - 1]
        g_dst[mine, :] = total * scale_dst
        for e in far_first:
            slot = h * (nz - 1) + e - 1
            c = rc(g_dst.at[mine, :], g_dst.at[mine, :], zs.at[slot], zr.at[slot], src=flip(e) * nx + b)
            c.start()
            zc[h, e] = c
        x_forward(h, 0)

    def forward(h):
        for e in far_first:
            zc[h, e].wait_recv()
            x_forward(h, e)

    q1c, q2c = [], []

    def project_all():
        left = far_first + [0]
        gacc = None
        thr[0] = through(group_of(0))
        for g, (side, oy) in enumerate(groups):
            first = group_of(g) * kd
            if g + 1 < nd:
                thr[(g + 1) % 2] = through(group_of(g + 1))
            for e in range(kd):
                th, tl = split(thr[g % 2, e * ni:(e + 1) * ni])
                wide = dg(sth, jnp.concatenate([th, tl], axis=1), 1, 0)
                proj[first + e] = wide[:, :r2n] + wide[:, r2n:] + dg(stl, th, 1, 0)
                term = dg(jnp.concatenate([th, tl, th], axis=1), chs[first + e], 1, 1)
                gacc = term if gacc is None else gacc + term
            core_of = lax.rem(cc + side, 2)
            peer = lax.rem(yy + oy, ny)
            if side:
                c = rc(proj.at[pl.ds(first, kd)], q1.at[peer], q1s.at[oy], q1r.at[oy], dst=2 * yy + core_of)
                c.start()
                q1c.append(c)
            else:
                q1c[oy - 1 if oy else ny - 1].wait_recv()
                q1[peer] = q1[peer] + proj[pl.ds(first, kd)]
                if oy:
                    c = rc(q1.at[peer], q2.at[oy - 1], q2s.at[oy - 1], q2r.at[oy - 1], dst=2 * peer + cc)
                    c.start()
                    q2c.append(c)
            if g == 0:
                for h in range(nh - 1):
                    for e in far_first + [0]:
                        z_send(h, e)
            else:
                for _ in range(len(left) // (nd - g)):
                    z_send(nh - 1, left.pop(0))
        gterm[...] = gacc

    count_copy(0).wait()
    misfit(0, 0)
    for t in range(nt):
        compute_block(t)
        if t == 0:
            pl.semaphore_wait(barrier, n - 1 + nd - 1)
        if t // nh < nx - 1:
            x_send(t % nh, t // nh)
    project_all()

    g1 = []
    for o in range(1, nd):
        peer = lax.rem(d + o, nd)
        c = rc(gterm.at[pl.ds(pl.multiple_of(peer * irows, irows), irows), :], r3.at[o - 1], gs1s.at[o - 1], gs1r.at[o - 1],
               dst=peer)
        c.start()
        g1.append(c)

    for h in range(nh - 1):
        finish(h)

    ysum = q1[yy]
    for o in range(1, ny):
        q2c[o - 1].wait_recv()
        ysum = ysum + q2[o - 1]
    for i in range(n):
        pq[i] = ysum[:, i * share:(i + 1) * share, :]
    q3c = []
    for o in range(1, n):
        peer = lax.rem(s + o, n)
        c = rc(pq.at[peer], q3.at[o - 1], q3s.at[o - 1], q3r.at[o - 1], src=peer)
        c.start()
        q3c.append(c)

    def hour_row(r, carry):
        for k in range(kk):
            acc = core[r, 0:8, :] * proj[k, 0:8, :]
            for i in range(1, r1n // 8):
                acc = acc + core[r, 8 * i:8 * i + 8, :] * proj[k, 8 * i:8 * i + 8, :]
            hacc[k, r] = acc
        return carry

    lax.fori_loop(0, r3n, hour_row, 0)
    hl = jnp.sum(jnp.sum(hacc[...], axis=2), axis=2)
    hl = jnp.concatenate([hl, jnp.zeros((kk, hd.shape[2] - r3n), F32)], axis=1)
    hd[d] = hl
    h1 = []
    for o in range(1, nd):
        c = rc(hd.at[d], hd.at[d], hds.at[o - 1], hdr.at[o - 1], dst=lax.rem(d + o, nd))
        c.start()
        h1.append(c)

    own_rows = pl.ds(pl.multiple_of(d * irows, irows), irows)
    gsum = gterm[own_rows, :]
    for o in range(1, nd):
        g1[o - 1].wait_recv()
        gsum = gsum + r3[o - 1]
    g_src[own_rows, :] = gsum * scale_src
    g2 = []
    for o in range(1, nd):
        c = rc(g_src.at[own_rows, :], g_src.at[own_rows, :], gs2s.at[o - 1], gs2r.at[o - 1], dst=lax.rem(d + o, nd))
        c.start()
        g2.append(c)

    finish(nh - 1)

    for o in range(1, nd):
        h1[o - 1].wait_recv()
    hsum = hd[0]
    for i in range(1, nd):
        hsum = hsum + hd[i]
    hs[s] = hsum
    h2 = []
    for o in range(1, n):
        c = rc(hs.at[s], hs.at[s], hss.at[o - 1], hsr.at[o - 1], src=lax.rem(s + o, n))
        c.start()
        h2.append(c)

    for h in range(nh):
        forward(h)

    psum = pq[s]
    for o in range(1, n):
        q3c[o - 1].wait_recv()
        psum = psum + q3[o - 1]
    pk[d] = psum
    pkc = []
    for o in range(1, nd):
        c = rc(pk.at[d], pk.at[d], pks.at[o - 1], pkr.at[o - 1], dst=lax.rem(d + o, nd))
        c.start()
        pkc.append(c)

    for o in range(1, n):
        h2[o - 1].wait_recv()
    htot = hs[0]
    for i in range(1, n):
        htot = htot + hs[i]
    g_hour[...] = htot[:, :r3n] * scale_hour

    for o in range(1, nd):
        pkc[o - 1].wait_recv()
    tiles = [pk[k // kd, k % kd] * scale_core for k in range(kk)]
    for r in range(r3n):
        acc = tiles[0] * hour[0, r]
        for k in range(1, kk):
            acc = acc + tiles[k] * hour[k, r]
        g_core[r] = acc

    for c in g2:
        c.wait_recv()
    for c in xc:
        c.wait_recv()
    for c in list(s1.values()) + list(s2.values()) + list(zc.values()) + xc + g1 + g2 + q1c + q2c + q3c + pkc + h1 + h2:
        c.wait_send()


def write_out(*refs):
    half = len(refs) // 3
    ins, outs, sems = refs[:half], refs[half:2 * half], refs[2 * half:]
    copies = [pltpu.make_async_copy(i, o, m) for i, o, m in zip(ins, outs, sems)]
    for c in copies:
        c.start()
    for c in copies:
        c.wait()


def solution(mesh):
    n = mesh.shape["src"]
    nd = mesh.shape["dst"]
    nx = 2 ** (int(math.log2(n)) // 2)
    nz = n // nx
    ny = nd // 2

    def shards(counts, src, dst, hour, core):
        kk, ni, nj = counts.shape
        r3n, r1n, r2n = core.shape
        tj = min(256, nj // nx)
        nh = nj // (nx * tj)
        kd = kk // nd
        share = r1n // n
        irows = ni // nd
        vm = pl.BlockSpec(memory_space=pltpu.VMEM)
        hbm = pl.BlockSpec(memory_space=pl.ANY)
        dma = lambda *shape: pltpu.SemaphoreType.DMA(shape)
        f = lambda *shape: pltpu.VMEM(shape, F32)
        h = lambda *shape: pltpu.VMEM(shape, BF16)
        pair = lambda m: [dma(m), dma(m)]
        scratch = [
            f(ni, r1n), f(nj, r2n), f(r3n, r1n, r2n), pltpu.VMEM((nh * nx, kk, ni, tj), jnp.int32),
            f(kk, r1n, r2n), h(kk, ni, 3 * r2n), h(kk, 2 * r2n, ni), h(3 * r2n, nj), h(nj, 2 * r2n),
            f(2, kd * ni, r2n), f(nj, r2n), f(nh * (nx - 1), tj, r2n), f(nh * (nz - 1), tj // nz, r2n),
            h(kk, r1n, 3 * r2n), f(ni, r1n), f(nd - 1, irows, r1n), f(kk, r1n, r2n), f(ny, kd, r1n, r2n), f(ny - 1, kd, r1n, r2n),
            f(n, kd, share, r2n), f(n - 1, kd, share, r2n), f(nd, kd, share, r2n), f(kk, r3n, 8, r2n),
            f(nd, kk, 128), f(n, kk, 128), h(nh * nx, nd, 2, kd * ni, tj),
            dma(3), dma(nh * nx),
        ]
        for m in (nh * (nx - 1) * nz, nh * (nz - 1), nh * (nz - 1), nh * (nx - 1) * nz, nd - 1, nd - 1, ny, ny - 1, n - 1, nd - 1, nd - 1, n - 1):
            scratch += pair(m)
        shapes = ((ni, r1n), (nj, r2n), (kk, r3n), (r3n, share, r2n))
        results = pl.pallas_call(
            functools.partial(kernel, n, nz, nx, nd, nh, tj),
            out_shape=tuple(pltpu.VMEM(x, F32) for x in shapes),
            in_specs=[hbm, hbm, hbm, pl.BlockSpec(memory_space=pltpu.SMEM), hbm],
            out_specs=(vm, vm, vm, vm),
            scratch_shapes=scratch,
            compiler_params=pltpu.CompilerParams(
                collective_id=0, has_side_effects=True, vmem_limit_bytes=60 * 1024 * 1024
            ),
        )(counts, src, dst, hour, core)
        return pl.pallas_call(
            write_out,
            out_shape=tuple(jax.ShapeDtypeStruct(x, F32) for x in shapes),
            in_specs=[vm] * 4,
            out_specs=(pl.BlockSpec(memory_space=pl.ANY),) * 4,
            scratch_shapes=[pltpu.SemaphoreType.DMA] * 4,
        )(*(pltpu.with_memory_space_constraint(x, pltpu.VMEM) for x in results))

    in_specs = (P(None, "src", "dst"), P("src", None), P("dst", None), P(), P())
    out_specs = (P("src", None), P("dst", None), P(), P(None, "src", None))
    return jax.shard_map(shards, mesh=mesh, in_specs=in_specs, out_specs=out_specs, check_vma=False)
```

```python
import functools
import math

import jax
import jax.numpy as jnp
from jax import lax
from jax.experimental import pallas as pl
from jax.experimental.pallas import tpu as pltpu
from jax.sharding import PartitionSpec as P

F32 = jnp.float32
BF16 = jnp.bfloat16
MESH = pl.DeviceIdType.MESH


def split(x):
    hi = x.astype(BF16)
    lo = (x - hi.astype(F32)).astype(BF16)
    return hi, lo


def dg(a, b, ca, cb):
    return lax.dot_general(a, b, (((ca,), (cb,)), ((), ())), preferred_element_type=F32)


def dot3(a, b, ca, cb):
    ah, al = a
    bh, bl = b
    return dg(ah, bh, ca, cb) + dg(ah, bl, ca, cb) + dg(al, bh, ca, cb)


def kernel(
    n, nz, nx, nd, nh, tj,
    counts, src_in, dst_in, hour, core_in,
    g_src, g_dst, g_hour, g_core,
    src, dst, core, cnt, ch, pf_ks, pf_t, d_k, d_n, thr, dacc, r1, r2,
    chs, gterm, r3, proj, q1, q2, pq, q3, pk, hacc, hd, hs, msc,
    i_sem, c_sem, s1s, s1r, s2s, s2r, zs, zr, xs, xr,
    gs1s, gs1r, gs2s, gs2r, q1s, q1r, q2s, q2r, q3s, q3r, pks, pkr, hds, hdr, hss, hsr,
):
    s = lax.axis_index("src")
    d = lax.axis_index("dst")
    a = s // nx
    b = lax.rem(s, nx)
    yy = d // 2
    cc = lax.rem(d, 2)
    ny = nd // 2
    kk, ni, _ = counts.shape
    nj = dst.shape[0]
    r3n = core.shape[0]
    r1n = core.shape[1]
    r2n = dst.shape[1]
    half = nj // nx
    zrows = tj // nz
    kd = kk // nd
    share = r1n // n
    irows = ni // nd
    nt = nh * nx
    scale_src = 1.0 / math.sqrt(nj * nd * kk)
    scale_dst = 1.0 / math.sqrt(ni * n * kk)
    scale_hour = 1.0 / math.sqrt(ni * n * nj * nd)
    scale_core = 1.0 / math.sqrt(ni * n * nj * nd * kk)

    dst_copy = pltpu.make_async_copy(dst_in, dst, i_sem.at[0])
    core_copy = pltpu.make_async_copy(core_in, core, i_sem.at[1])
    src_copy = pltpu.make_async_copy(src_in, src, i_sem.at[2])
    for c in (dst_copy, core_copy, src_copy):
        c.start()

    def block_start(t):
        return lax.rem(b + 1 + t // nh, nx) * half + (t % nh) * tj

    def flip(e):
        out = a
        for bit in range(e.bit_length()):
            if (e >> bit) % 2:
                out = out + (1 << bit) * (1 - 2 * lax.rem(a // (1 << bit), 2))
        return out

    far_first = list(range(nz - 1, 0, -1))

    def count_copy(t):
        start = pl.multiple_of(block_start(t), tj)
        return pltpu.make_async_copy(counts.at[:, :, pl.ds(start, tj)], cnt.at[t], c_sem.at[t])

    for t in range(nt):
        count_copy(t).start()

    barrier = pltpu.get_barrier_semaphore()
    for o in range(1, n):
        pl.semaphore_signal(barrier, inc=1, device_id={"src": lax.rem(s + o, n)}, device_id_type=MESH)
    for o in range(1, nd):
        pl.semaphore_signal(barrier, inc=1, device_id={"dst": lax.rem(d + o, nd)}, device_id_type=MESH)

    def rc(src_ref, dst_ref, send, recv, **where):
        return pltpu.make_async_remote_copy(
            src_ref=src_ref, dst_ref=dst_ref, send_sem=send, recv_sem=recv,
            device_id=where, device_id_type=MESH,
        )

    dst_copy.wait()
    dh, dl = split(dst[...])
    d_n[...] = jnp.concatenate([dh, dl], axis=1)
    dth, dtl = split(dst[...].T)
    d_k[...] = jnp.concatenate([dth, dth, dtl], axis=0)

    core_copy.wait()
    pt = 32

    def core_tile(i, carry):
        at = pl.ds(pl.multiple_of(i * pt, pt), pt)
        accs = [None] * kk
        for r in range(r3n):
            tile = core[r, at, :]
            for k in range(kk):
                term = tile * hour[k, r]
                accs[k] = term if r == 0 else accs[k] + term
        for k in range(kk):
            ch[k, at, :] = accs[k]
        return carry

    lax.fori_loop(0, r1n // pt, core_tile, 0)

    src_copy.wait()
    src_parts = split(src[...])

    def fit_one(k, carry):
        chh, chl = split(ch[k])
        chs[k] = jnp.concatenate([chh, chh, chl], axis=1)
        pf = dot3(src_parts, (chh, chl), 1, 0)
        ph, plo = split(pf)
        pf_ks[k] = jnp.concatenate([ph, plo, ph], axis=1)
        th, tl = split(pf.T)
        pf_t[k] = jnp.concatenate([th, tl], axis=0)
        return carry

    lax.fori_loop(0, kk, fit_one, 0)
    sth, stl = split(src[...].T)

    def misfit(t, g):
        at = pl.ds(pl.multiple_of(block_start(t), tj), tj)
        hours = slice(g * kd, (g + 1) * kd)
        fitted = dg(pf_ks[hours].reshape(kd * ni, 3 * r2n), d_k[:, at], 1, 0)
        m = 1.0 - cnt[t, hours].reshape(kd * ni, tj).astype(F32) / fitted
        mh, ml = split(m)
        msc[t, g, 0] = mh
        msc[t, g, 1] = ml

    def add_tall(t, g, acc):
        for e in range(kd):
            pt_ = pf_t[g * kd + e]
            rows = slice(e * ni, (e + 1) * ni)
            tall = dg(pt_, msc[t, g, 0, rows], 1, 0)
            new = tall[:r2n] + tall[r2n:] + dg(pt_[:r2n], msc[t, g, 1, rows], 1, 0)
            acc = new if acc is None else acc + new
        return acc

    def through(gi):
        out = None
        for t in range(nt):
            dn = d_n[pl.ds(pl.multiple_of(block_start(t), tj), tj), :]
            wide = dg(msc[t, gi, 0], dn, 1, 0)
            new = wide[:, :r2n] + wide[:, r2n:] + dg(msc[t, gi, 1], dn[:, :r2n], 1, 0)
            out = new if out is None else out + new
        return out

    groups = [(side, oy) for oy in list(range(1, ny)) + [0] for side in (1, 0)]

    def group_of(g):
        side, oy = groups[g]
        return 2 * lax.rem(yy + oy, ny) + lax.rem(cc + side, 2)

    def compute_block(t):
        if t + 1 < nt:
            count_copy(t + 1).wait()
        acc = None
        for g in range(nd):
            if g + 1 < nd:
                misfit(t, g + 1)
            elif t + 1 < nt:
                misfit(t + 1, 0)
            acc = add_tall(t, g, acc)
        dacc[pl.ds(pl.multiple_of(block_start(t), tj), tj), :] = acc.T

    s1, s2, zc, xc = {}, {}, {}, []

    def x_send(h, step):
        start = block_start(step * nh + h)
        slot = h * (nx - 1) + step
        for e in far_first + [0]:
            at = flip(e) * zrows
            c = rc(dacc.at[pl.ds(pl.multiple_of(start + at, zrows), zrows), :],
                   r1.at[slot, pl.ds(pl.multiple_of(at, zrows), zrows), :],
                   s1s.at[slot * nz + e], s1r.at[slot * nz + e], src=a * nx + lax.rem(b + 1 + step, nx))
            c.start()
            s1[slot, e] = c

    def z_piece(h, owner):
        return pl.ds(pl.multiple_of(b * half + h * tj + owner * zrows, zrows), zrows)

    def z_send(h, e):
        owner = flip(e)
        at = z_piece(h, owner)
        value = dacc[at, :]
        for step in range(nx - 1):
            s1[h * (nx - 1) + step, e].wait_recv()
            value = value + r1[h * (nx - 1) + step, pl.ds(pl.multiple_of(owner * zrows, zrows), zrows), :]
        dacc[at, :] = value
        if e:
            slot = h * (nz - 1) + e - 1
            c = rc(dacc.at[at, :], r2.at[slot], s2s.at[slot], s2r.at[slot], src=owner * nx + b)
            c.start()
            s2[h, e] = c

    def x_copy(h, step, o):
        at = z_piece(h, flip(o))
        slot = (h * (nx - 1) + step) * nz + o
        return rc(g_dst.at[at, :], g_dst.at[at, :], xs.at[slot], xr.at[slot],
                  src=a * nx + lax.rem(b + 1 + step, nx))

    def x_forward(h, o):
        for step in range(nx - 1):
            c = x_copy(h, step, o)
            c.start()
            xc.append(c)

    def finish(h):
        mine = z_piece(h, a)
        total = dacc[mine, :]
        for e in far_first:
            s2[h, e].wait_recv()
            total = total + r2[h * (nz - 1) + e - 1]
        g_dst[mine, :] = total * scale_dst
        for e in far_first:
            slot = h * (nz - 1) + e - 1
            c = rc(g_dst.at[mine, :], g_dst.at[mine, :], zs.at[slot], zr.at[slot], src=flip(e) * nx + b)
            c.start()
            zc[h, e] = c
        x_forward(h, 0)

    def forward(h):
        for e in far_first:
            zc[h, e].wait_recv()
            x_forward(h, e)

    q1c, q2c = [], []

    def project_all():
        left = far_first + [0]
        gacc = None
        thr[0] = through(group_of(0))
        for g, (side, oy) in enumerate(groups):
            first = group_of(g) * kd
            if g + 1 < nd:
                thr[(g + 1) % 2] = through(group_of(g + 1))
            for e in range(kd):
                th, tl = split(thr[g % 2, e * ni:(e + 1) * ni])
                wide = dg(sth, jnp.concatenate([th, tl], axis=1), 1, 0)
                proj[first + e] = wide[:, :r2n] + wide[:, r2n:] + dg(stl, th, 1, 0)
                term = dg(jnp.concatenate([th, tl, th], axis=1), chs[first + e], 1, 1)
                gacc = term if gacc is None else gacc + term
            core_of = lax.rem(cc + side, 2)
            peer = lax.rem(yy + oy, ny)
            if side:
                c = rc(proj.at[pl.ds(first, kd)], q1.at[peer], q1s.at[oy], q1r.at[oy], dst=2 * yy + core_of)
                c.start()
                q1c.append(c)
            else:
                q1c[oy - 1 if oy else ny - 1].wait_recv()
                q1[peer] = q1[peer] + proj[pl.ds(first, kd)]
                if oy:
                    c = rc(q1.at[peer], q2.at[oy - 1], q2s.at[oy - 1], q2r.at[oy - 1], dst=2 * peer + cc)
                    c.start()
                    q2c.append(c)
            if g == 0:
                for h in range(nh - 1):
                    for e in far_first + [0]:
                        z_send(h, e)
            else:
                for _ in range(len(left) // (nd - g)):
                    z_send(nh - 1, left.pop(0))
        gterm[...] = gacc

    count_copy(0).wait()
    misfit(0, 0)
    for t in range(nt):
        compute_block(t)
        if t == 0:
            pl.semaphore_wait(barrier, n - 1 + nd - 1)
        if t // nh < nx - 1:
            x_send(t % nh, t // nh)
    project_all()

    g1 = []
    for o in range(1, nd):
        peer = lax.rem(d + o, nd)
        c = rc(gterm.at[pl.ds(pl.multiple_of(peer * irows, irows), irows), :], r3.at[o - 1], gs1s.at[o - 1], gs1r.at[o - 1],
               dst=peer)
        c.start()
        g1.append(c)

    for h in range(nh - 1):
        finish(h)

    ysum = q1[yy]
    for o in range(1, ny):
        q2c[o - 1].wait_recv()
        ysum = ysum + q2[o - 1]
    for i in range(n):
        pq[i] = ysum[:, i * share:(i + 1) * share, :]
    q3c = []
    for o in range(1, n):
        peer = lax.rem(s + o, n)
        c = rc(pq.at[peer], q3.at[o - 1], q3s.at[o - 1], q3r.at[o - 1], src=peer)
        c.start()
        q3c.append(c)

    def hour_row(r, carry):
        for k in range(kk):
            acc = core[r, 0:8, :] * proj[k, 0:8, :]
            for i in range(1, r1n // 8):
                acc = acc + core[r, 8 * i:8 * i + 8, :] * proj[k, 8 * i:8 * i + 8, :]
            hacc[k, r] = acc
        return carry

    lax.fori_loop(0, r3n, hour_row, 0)
    hl = jnp.sum(jnp.sum(hacc[...], axis=2), axis=2)
    hl = jnp.concatenate([hl, jnp.zeros((kk, hd.shape[2] - r3n), F32)], axis=1)
    hd[d] = hl
    h1 = []
    for o in range(1, nd):
        c = rc(hd.at[d], hd.at[d], hds.at[o - 1], hdr.at[o - 1], dst=lax.rem(d + o, nd))
        c.start()
        h1.append(c)

    own_rows = pl.ds(pl.multiple_of(d * irows, irows), irows)
    gsum = gterm[own_rows, :]
    for o in range(1, nd):
        g1[o - 1].wait_recv()
        gsum = gsum + r3[o - 1]
    g_src[own_rows, :] = gsum * scale_src
    g2 = []
    for o in range(1, nd):
        c = rc(g_src.at[own_rows, :], g_src.at[own_rows, :], gs2s.at[o - 1], gs2r.at[o - 1], dst=lax.rem(d + o, nd))
        c.start()
        g2.append(c)

    finish(nh - 1)

    for o in range(1, nd):
        h1[o - 1].wait_recv()
    hsum = hd[0]
    for i in range(1, nd):
        hsum = hsum + hd[i]
    hs[s] = hsum
    h2 = []
    for o in range(1, n):
        c = rc(hs.at[s], hs.at[s], hss.at[o - 1], hsr.at[o - 1], src=lax.rem(s + o, n))
        c.start()
        h2.append(c)

    for h in range(nh):
        forward(h)

    psum = pq[s]
    for o in range(1, n):
        q3c[o - 1].wait_recv()
        psum = psum + q3[o - 1]
    pk[d] = psum
    pkc = []
    for o in range(1, nd):
        c = rc(pk.at[d], pk.at[d], pks.at[o - 1], pkr.at[o - 1], dst=lax.rem(d + o, nd))
        c.start()
        pkc.append(c)

    for o in range(1, n):
        h2[o - 1].wait_recv()
    htot = hs[0]
    for i in range(1, n):
        htot = htot + hs[i]
    g_hour[...] = htot[:, :r3n] * scale_hour

    for o in range(1, nd):
        pkc[o - 1].wait_recv()
    tiles = [pk[k // kd, k % kd] * scale_core for k in range(kk)]
    for r in range(r3n):
        acc = tiles[0] * hour[0, r]
        for k in range(1, kk):
            acc = acc + tiles[k] * hour[k, r]
        g_core[r] = acc

    for c in g2:
        c.wait_recv()
    for c in xc:
        c.wait_recv()
    for c in list(s1.values()) + list(s2.values()) + list(zc.values()) + xc + g1 + g2 + q1c + q2c + q3c + pkc + h1 + h2:
        c.wait_send()


def write_out(*refs):
    half = len(refs) // 3
    ins, outs, sems = refs[:half], refs[half:2 * half], refs[2 * half:]
    copies = [pltpu.make_async_copy(i, o, m) for i, o, m in zip(ins, outs, sems)]
    for c in copies:
        c.start()
    for c in copies:
        c.wait()


def solution(mesh):
    n = mesh.shape["src"]
    nd = mesh.shape["dst"]
    nx = 2 ** (int(math.log2(n)) // 2)
    nz = n // nx
    ny = nd // 2

    def shards(counts, src, dst, hour, core):
        kk, ni, nj = counts.shape
        r3n, r1n, r2n = core.shape
        tj = min(256, nj // nx)
        nh = nj // (nx * tj)
        kd = kk // nd
        share = r1n // n
        irows = ni // nd
        vm = pl.BlockSpec(memory_space=pltpu.VMEM)
        hbm = pl.BlockSpec(memory_space=pl.ANY)
        dma = lambda *shape: pltpu.SemaphoreType.DMA(shape)
        f = lambda *shape: pltpu.VMEM(shape, F32)
        h = lambda *shape: pltpu.VMEM(shape, BF16)
        pair = lambda m: [dma(m), dma(m)]
        scratch = [
            f(ni, r1n), f(nj, r2n), f(r3n, r1n, r2n), pltpu.VMEM((nh * nx, kk, ni, tj), jnp.int32),
            f(kk, r1n, r2n), h(kk, ni, 3 * r2n), h(kk, 2 * r2n, ni), h(3 * r2n, nj), h(nj, 2 * r2n),
            f(2, kd * ni, r2n), f(nj, r2n), f(nh * (nx - 1), tj, r2n), f(nh * (nz - 1), tj // nz, r2n),
            h(kk, r1n, 3 * r2n), f(ni, r1n), f(nd - 1, irows, r1n), f(kk, r1n, r2n), f(ny, kd, r1n, r2n), f(ny - 1, kd, r1n, r2n),
            f(n, kd, share, r2n), f(n - 1, kd, share, r2n), f(nd, kd, share, r2n), f(kk, r3n, 8, r2n),
            f(nd, kk, 128), f(n, kk, 128), h(nh * nx, nd, 2, kd * ni, tj),
            dma(3), dma(nh * nx),
        ]
        for m in (nh * (nx - 1) * nz, nh * (nz - 1), nh * (nz - 1), nh * (nx - 1) * nz, nd - 1, nd - 1, ny, ny - 1, n - 1, nd - 1, nd - 1, n - 1):
            scratch += pair(m)
        shapes = ((ni, r1n), (nj, r2n), (kk, r3n), (r3n, share, r2n))
        results = pl.pallas_call(
            functools.partial(kernel, n, nz, nx, nd, nh, tj),
            out_shape=tuple(pltpu.VMEM(x, F32) for x in shapes),
            in_specs=[hbm, hbm, hbm, pl.BlockSpec(memory_space=pltpu.SMEM), hbm],
            out_specs=(vm, vm, vm, vm),
            scratch_shapes=scratch,
            compiler_params=pltpu.CompilerParams(
                collective_id=0, has_side_effects=True, vmem_limit_bytes=60 * 1024 * 1024
            ),
        )(counts, src, dst, hour, core)
        return pl.pallas_call(
            write_out,
            out_shape=tuple(jax.ShapeDtypeStruct(x, F32) for x in shapes),
            in_specs=[vm] * 4,
            out_specs=(pl.BlockSpec(memory_space=pl.ANY),) * 4,
            scratch_shapes=[pltpu.SemaphoreType.DMA] * 4,
        )(*(pltpu.with_memory_space_constraint(x, pltpu.VMEM) for x in results))

    in_specs = (P(None, "src", "dst"), P("src", None), P("dst", None), P(), P())
    out_specs = (P("src", None), P("dst", None), P(), P(None, "src", None))
    return jax.shard_map(shards, mesh=mesh, in_specs=in_specs, out_specs=out_specs, check_vma=False)
```
